32 devices in a mesh: dp: 4 (over y, x), vocab: 8 (over z, core).
Axes of the slice: x: 2, y: 2, z: 4, core: 2. Of those that a mesh axis runs over, the one named last changes fastest.
Arguments:
- hidden: bfloat16 [4, 32, 3584], P('dp', None, 'vocab'), may hold values from -6 to 6
- kl_hidden: bfloat16 [4, 32, 3584], P('dp', None, 'vocab'), may hold values from -6 to 6
- head_weight: bfloat16 [256000, 3584], P(('dp', 'vocab')), may hold values from -0.3125 to 0.3125
- labels: int32 [4, 32], P('dp'), may hold values from 0 to 255999
- token_mask: int32 [4, 32], P('dp'), may hold values 0 or 1
- kl_pair: int32 [4], P('dp'), may hold values from 0 to 3, as said below
- desirable: int32 [4], P('dp'), may hold values 0 or 1
- ref_logps: float32 [4, 64], P('dp', 'vocab'), may hold values from -23 to -11
Outputs:
- token_logps: float32 [4, 64], P('dp', 'vocab')
- seq_losses: float32 [4], P('dp')
- loss: float32 [], replicated
The draws below stay inside these ranges and needn't reach their ends.
Inputs may be any that keep to these rules, and one draw needn't show every extreme that they name: kl_pair is a permutation of the 4 sequences with kl_pair[s] != s.
All inputs are finite; a program needn't handle non-finite values. No bound on the sum of `token_mask` or of `desirable` on one device may be relied on, other than what follows from the above.
Results may differ from the reference program's by a relative error of at most 0.0003.
Values may be sent and summed in bfloat16 or wider, within the bound.
A program may use at most 128 MiB of HBM per device.

```python
import jax
import jax.numpy as jnp
from jax import lax

D = 3584
V = 256000
LEN = 32
SEQS = 4


def draw_kl_pair(key, part):
    order = jax.random.permutation(jax.random.fold_in(key, 7), SEQS).astype(jnp.int32)
    placing = jnp.argsort(order, stable=True).astype(jnp.int32)
    return order[(placing + 1) % SEQS].astype(jnp.int32)


def with_ends(array, rng, low, top_value):
    spot = [jax.random.randint(jax.random.fold_in(rng, axis), (), 0, length) for axis, length in enumerate(array.shape)]
    widest = array.shape.index(max(array.shape))
    neighbour = spot[:widest] + [(spot[widest] + 1) % array.shape[widest]] + spot[widest + 1:]
    return array.at[tuple(spot)].set(low).at[tuple(neighbour)].set(top_value)


def levels(key, dims, cuts, least, largest):
    loudness, own = 1.0, jax.random.fold_in(key, 6)
    for axis_at, parts in cuts:
        steps = jnp.exp(jax.random.uniform(jax.random.fold_in(own, axis_at), (parts,), jnp.float32, least / len(cuts), largest / len(cuts)))
        loudness = loudness * jnp.repeat(steps, dims[axis_at] // parts).reshape([-1 if axis == axis_at else 1 for axis in range(len(dims))])
    return loudness


def normal_values(stream_key, shape, deviation, limit, shards=(), held_as=jnp.bfloat16):
    level = levels(stream_key, shape, shards, -0.22, 0.18) if shards else 1.0
    array = jax.random.normal(stream_key, shape, jnp.float32) * deviation * level
    return jnp.minimum(jnp.maximum(array, -limit), limit).astype(held_as)


def setup_inputs(seed: int = 0) -> dict:
    streams_of = jax.random.split(jax.random.key(seed), 9)
    hidden = normal_values(streams_of[0], (SEQS, LEN, D), 1.0, 6.0, ((0, 4), (2, 8)))
    kl_hidden = normal_values(streams_of[1], (SEQS, LEN, D), 1.0, 6.0, ((0, 4), (2, 8)))
    head_weight = normal_values(streams_of[2], (V, D), (D // 9) ** -0.5, 0.3125, ((0, 32),))
    labels = with_ends(jax.random.randint(streams_of[3], (SEQS, LEN), 0, V), jax.random.fold_in(streams_of[3], 1), 0, V - 1).astype(jnp.int32)
    token_mask = with_ends((jax.random.randint(streams_of[4], (SEQS, LEN), 0, 4) < 3).astype(jnp.int32), jax.random.fold_in(streams_of[4], 1), 0, 1)
    kl_pair = draw_kl_pair(jax.random.fold_in(streams_of[8], 71), 0)
    desirable = with_ends((jax.random.randint(streams_of[6], (SEQS,), 0, 2) < 1).astype(jnp.int32), jax.random.fold_in(streams_of[6], 1), 0, 1)
    ref_logps = jnp.clip(-23.0 + 12.0 * jax.random.uniform(streams_of[7], (SEQS, 2 * LEN), jnp.float32) ** levels(streams_of[7], (SEQS, 2 * LEN), ((0, 4), (1, 8)), -0.2, 0.2), -23.0, -11.0)
    return dict(hidden=hidden, kl_hidden=kl_hidden, head_weight=head_weight, labels=labels, token_mask=token_mask, kl_pair=kl_pair, desirable=desirable, ref_logps=ref_logps)


kto_beta = 0.1
desirable_weight = 1.0
undesirable_weight = 1.33


def reference(hidden, kl_hidden, head_weight, labels, token_mask, kl_pair, desirable, ref_logps):
    all_rows = jnp.concatenate([hidden, kl_hidden], axis=1).reshape(-1, D)
    targets = jnp.concatenate([labels, labels[kl_pair]], axis=1)
    weights_mask = jnp.concatenate([token_mask, token_mask[kl_pair]], axis=1).astype(jnp.float32)
    block_rows = V // 32
    blocks = head_weight.reshape(32, block_rows, D)

    def add_block(running, wblock):
        logits = lax.dot_general(all_rows, wblock, (((1,), (1,)), ((), ())), preferred_element_type=jnp.float32)
        return running + jnp.sum(jnp.exp(logits), axis=1), None

    partition, unused = lax.scan(add_block, jnp.zeros((all_rows.shape[0],), jnp.float32), blocks)
    target_rows = head_weight[targets.reshape(-1)].astype(jnp.float32)
    picked = jnp.sum(all_rows.astype(jnp.float32) * target_rows, axis=1)
    token_logps = (picked - jnp.log(partition)).reshape(SEQS, 2 * LEN)
    differences = weights_mask * (token_logps - ref_logps)
    logratio = jnp.sum(differences[:, :LEN], axis=1)
    kl_terms = jnp.sum(differences[:, LEN:], axis=1)
    kl_estimate = jnp.mean(kl_terms)
    wanted = desirable_weight * (1.0 - jax.nn.sigmoid(kto_beta * (logratio - kl_estimate)))
    unwanted = undesirable_weight * (1.0 - jax.nn.sigmoid(kto_beta * (kl_estimate - logratio)))
    seq_losses = jnp.where(desirable == 1, wanted, unwanted)
    return token_logps, seq_losses, jnp.mean(seq_losses)
```

```python
import functools

import jax
import jax.numpy as jnp
from jax import lax
from jax.experimental import pallas as pl
from jax.experimental.pallas import tpu as pltpu
from jax.sharding import PartitionSpec as P

MESH = pl.DeviceIdType.MESH
LANES = 128
TILE_ROWS = 2000


kto_beta = 0.1
desirable_weight = 1.0
undesirable_weight = 1.33


def label_terms(logits, targets, first_row):
    shifted = targets - first_row
    inside = (shifted >= 0) & (shifted < logits.shape[1])
    clipped = jnp.clip(shifted, 0, logits.shape[1] - 1)
    picked = jnp.take_along_axis(logits, clipped[:, None], axis=1)[:, 0]
    return (jnp.sum(jnp.exp(logits), axis=1), jnp.where(inside, picked, 0.0))


def kto_losses(logratio, kl_total, seq_total, desirable):
    kl_estimate = kl_total / seq_total
    wanted = desirable_weight * (1.0 - jax.nn.sigmoid(kto_beta * (logratio - kl_estimate)))
    unwanted = undesirable_weight * (1.0 - jax.nn.sigmoid(kto_beta * (kl_estimate - logratio)))
    return jnp.where(desirable == 1, wanted, unwanted)


def gathered_by_xla(hidden, kl_hidden, head_weight, labels, token_mask, kl_pair, desirable, ref_logps):
    sub_seq = hidden.shape[0]
    length = hidden.shape[1]
    vocab_rows = head_weight.shape[0]
    model_width = head_weight.shape[1]
    groups = lax.axis_size("vocab")
    vocab_index = lax.axis_index("vocab")
    data_index = lax.axis_index("dp")
    first_row = (data_index * groups + vocab_index) * vocab_rows
    all_labels, all_masks, all_pairs, all_desirable = (
        lax.all_gather(labels, "dp", axis=0, tiled=True),
        lax.all_gather(token_mask, "dp", axis=0, tiled=True),
        lax.all_gather(kl_pair, "dp", axis=0, tiled=True),
        lax.all_gather(desirable, "dp", axis=0, tiled=True),
    )
    targets = jnp.concatenate([all_labels, all_labels[all_pairs]], axis=1)
    weights_mask = jnp.concatenate([all_masks, all_masks[all_pairs]], axis=1).astype(jnp.float32)
    seq_total = targets.shape[0]
    columns = targets.shape[1]
    combined = jnp.concatenate([hidden, kl_hidden], axis=1)
    whole_rows = lax.all_gather(combined, "vocab", axis=2, tiled=True)
    portion = lax.all_gather(whole_rows, "dp", axis=0, tiled=True)
    number = portion.shape[0]
    logits = lax.dot_general(
        portion.reshape(number * columns, model_width),
        head_weight,
        (((1,), (1,)), ((), ())),
        preferred_element_type=jnp.float32,
    )
    portion_targets = targets.reshape(-1)
    part_sum, part_pick = label_terms(logits, portion_targets, first_row)
    token_stats = jnp.stack(
        [part_sum.reshape(number, columns), part_pick.reshape(number, columns)], axis=1
    )
    partition = token_stats[:, 0]
    picked = token_stats[:, 1]
    own_cols = columns // groups
    row_start = data_index * sub_seq
    col_start = vocab_index * own_cols
    ref_full = lax.dynamic_update_slice(
        jnp.zeros((seq_total, columns), jnp.float32), ref_logps, (row_start, col_start)
    )
    partition, picked, ref_all = lax.psum((partition, picked, ref_full), ("dp", "vocab"))
    token_logps = picked - jnp.log(partition)
    differences = weights_mask * (token_logps - ref_all)
    logratio = jnp.sum(differences[:, :length], axis=1)
    kl_terms = jnp.sum(differences[:, length:], axis=1)
    losses = kto_losses(logratio, jnp.sum(kl_terms), seq_total, all_desirable)
    own_logps = lax.dynamic_slice(token_logps, (row_start, col_start), (sub_seq, own_cols))
    own_losses = lax.dynamic_slice_in_dim(losses, row_start, sub_seq, 0)
    return (own_logps, own_losses, jnp.mean(losses))


def fused_kernel(dims, hid, klh, weight, labels, mask, pair, flag, ref, out, held, wbuf, acc, xeven, xodd,
                 lab_v, mask_v, pair_v, flag_v, ref_v, meta, sums, picks, red, xs, ms, ws, ici, d2d,
                 s_plane, s_part, s_right, s_left, m_send, m_recv, r_send, r_recv):
    seqs, groups = dims
    depth = groups // 2
    devices = seqs * groups
    length = hid.shape[1]
    columns = 2 * length
    width = hid.shape[2]
    chunk = 2 * width
    vocab_rows = weight.shape[0]
    tile = TILE_ROWS
    tiles = vocab_rows // tile
    positions = seqs * columns
    d = lax.axis_index("dp")
    v = lax.axis_index("vocab")
    z = lax.div(v, 2)
    c = lax.rem(v, 2)
    me = d * groups + v
    partner = (d, z * 2 + (1 - c))
    above = (d, jnp.minimum(v + 2, groups - 1))
    below = (d, jnp.maximum(v - 2, 0))
    has_above = z + 1 < depth
    has_below = z >= 1

    def order(step):
        least = jnp.minimum(z, depth - 1 - z)
        near = (step + 1) // 2
        inner = z - near if step % 2 else z + near
        outer = jnp.where(z > depth - 1 - z, z - (step - least), z + (step - least))
        return jnp.where(step <= 2 * least, inner, outer)

    chunks = [order(step) for step in range(depth)]

    def block(parity, zc, dc):
        return held.at[parity, zc, pl.ds(pl.multiple_of(dc * columns, columns), columns)]

    def weight_copies(p, i):
        rows = pl.ds(pl.multiple_of(i * tile, tile), tile)
        base = pl.multiple_of(chunks[p] * chunk, LANES)
        if p % 2 == 0:
            return [pltpu.make_async_copy(weight.at[rows, pl.ds(base, chunk - LANES)],
                                          wbuf.at[rows, pl.ds(0, chunk - LANES)], ws.at[i, 0])]
        last = pl.multiple_of(chunks[p - 1] * chunk + chunk - LANES, LANES)
        return [
            pltpu.make_async_copy(weight.at[rows, pl.ds(last, LANES)], wbuf.at[rows, pl.ds(0, LANES)], ws.at[i, 0]),
            pltpu.make_async_copy(weight.at[rows, pl.ds(base, chunk)], wbuf.at[rows, pl.ds(LANES, chunk)], ws.at[i, 1]),
        ]

    def send(src, dst, send_sem, recv_sem, device):
        return pltpu.make_async_remote_copy(src_ref=src, dst_ref=dst, send_sem=send_sem, recv_sem=recv_sem,
                                            device_id=device, device_id_type=MESH)

    def to_plane(k):
        return send(block(c, z, d), block(c, z, d), s_plane.at[k], ici.at[z, d], (lax.rem(d + k, seqs), v))

    def meta_to(k):
        return send(meta.at[d], meta.at[d], m_send.at[k], m_recv.at[d], (lax.rem(d + k, seqs), v))

    def to_partner(zc, dc):
        return send(block(c, zc, dc), block(c, zc, dc), s_part.at[zc, dc], d2d.at[zc, dc], partner)

    def to_above(zc, dc):
        return send(block(c, zc, dc), block(c, zc, dc), s_right.at[zc, dc], ici.at[zc, dc], above)

    def to_below(zc, dc):
        return send(block(c, zc, dc), block(c, zc, dc), s_left.at[zc, dc], ici.at[zc, dc], below)

    def from_ici(zc, dc):
        return send(block(c, zc, dc), block(c, zc, dc), s_part.at[zc, dc], ici.at[zc, dc], partner)

    def from_partner(zc, dc):
        return send(block(1 - c, zc, dc), block(1 - c, zc, dc), s_part.at[zc, dc], d2d.at[zc, dc], partner)

    small = [
        pltpu.make_async_copy(labels, lab_v, ms.at[0]),
        pltpu.make_async_copy(mask, mask_v, ms.at[1]),
        pltpu.make_async_copy(pair, pair_v, ms.at[2]),
        pltpu.make_async_copy(flag, flag_v, ms.at[3]),
        pltpu.make_async_copy(ref, ref_v, ms.at[4]),
    ]
    own_rows = [
        pltpu.make_async_copy(hid.at[0], held.at[c, z, pl.ds(pl.multiple_of(d * columns, columns), length)], xs.at[0]),
        pltpu.make_async_copy(
            klh.at[0], held.at[c, z, pl.ds(pl.multiple_of(d * columns + length, length), length)], xs.at[1]),
    ]

    barrier = pltpu.get_barrier_semaphore()
    for copy in own_rows + small:
        copy.start()
    for k in range(1, seqs):
        pl.semaphore_signal(barrier, inc=1, device_id=(lax.rem(d + k, seqs), v), device_id_type=MESH)
    pl.semaphore_signal(barrier, inc=1, device_id=partner, device_id_type=MESH)

    @pl.when(has_above)
    def _():
        pl.semaphore_signal(barrier, inc=1, device_id=above, device_id_type=MESH)

    @pl.when(has_below)
    def _():
        pl.semaphore_signal(barrier, inc=1, device_id=below, device_id_type=MESH)

    def first_weights(i, carry):
        for copy in weight_copies(0, i):
            copy.start()
        return carry

    lax.fori_loop(0, tiles, first_weights, 0)
    for copy in own_rows + small:
        copy.wait()
    meta[d] = jnp.zeros((8, LANES), jnp.int32)
    meta[d, 0:1, 0:length] = lab_v[...]
    meta[d, 1:2, 0:length] = mask_v[...]
    meta[d, 2:3, :] = jnp.broadcast_to(pair_v[...], (1, LANES))
    meta[d, 3:4, :] = jnp.broadcast_to(flag_v[...], (1, LANES))
    pl.semaphore_wait(barrier, seqs + has_above.astype(jnp.int32) + has_below.astype(jnp.int32))

    for k in range(1, seqs):
        to_plane(k).start()
    to_partner(z, d).start()

    @pl.when(has_above)
    def _():
        to_above(z, d).start()

    @pl.when(has_below)
    def _():
        to_below(z, d).start()

    for k in (1, 2, 3) if seqs == 4 else range(1, seqs):
        dk = lax.rem(d + seqs - k, seqs)
        from_ici(z, dk).wait_recv()
        to_partner(z, dk).start()

        @pl.when(has_above)
        def _():
            to_above(z, dk).start()

        @pl.when(has_below)
        def _():
            to_below(z, dk).start()

    for k in range(1, seqs):
        meta_to(k).start()

    def relay(step):
        @pl.when(z - step >= 0)
        def _():
            for dc in range(seqs):
                from_ici(z - step, dc).wait_recv()
                to_partner(z - step, dc).start()

                @pl.when(has_above)
                def _():
                    to_above(z - step, dc).start()

        @pl.when(z + step < depth)
        def _():
            for dc in range(seqs):
                from_ici(z + step, dc).wait_recv()
                to_partner(z + step, dc).start()

                @pl.when(has_below)
                def _():
                    to_below(z + step, dc).start()

    def whole_chunk(zc):
        for dc in range(seqs):
            from_partner(zc, dc).wait_recv()
        return jnp.concatenate([held[0, zc], held[1, zc]], axis=1)

    lane = lax.broadcasted_iota(jnp.int32, (1, LANES), 1)
    first_row = me * vocab_rows

    def spread(row):
        own = [meta[s, row:row + 1, :] for s in range(seqs)]
        parts = []
        for s in range(seqs):
            which = meta[s, 2:3, :]
            other = jnp.zeros((1, LANES), jnp.int32)
            for t in range(seqs):
                other = jnp.where(which == t, own[t], other)
            parts.append(jnp.where(lane < length, own[s], pltpu.roll(other, length, 1)))
        return jnp.concatenate(
            [jnp.where(lane < columns, parts[s], pltpu.roll(parts[s + 1], columns, 1)) for s in range(0, seqs, 2)],
            axis=1)

    for p in range(depth):
        rows = whole_chunk(chunks[p])
        if p % 2 == 0:
            xeven[...] = rows
            deep = chunk - LANES
            x_ref = xeven
        else:
            xodd[:, 0:LANES] = xeven[:, chunk - LANES:chunk]
            xodd[:, LANES:chunk + LANES] = rows
            deep = chunk + LANES
            x_ref = xodd
        final = p == depth - 1
        if final:
            for k in range(1, seqs):
                dk = lax.rem(d + seqs - k, seqs)
                send(meta.at[dk], meta.at[dk], m_send.at[k], m_recv.at[dk], partner).wait_recv()
            targets = spread(0) - first_row
            sums[...] = jnp.zeros_like(sums)
            picks[...] = jnp.zeros_like(picks)

        def one_tile(i, carry, p=p, deep=deep, x_ref=x_ref, final=final):
            at = pl.ds(pl.multiple_of(i * tile, tile), tile)
            for copy in weight_copies(p, i):
                copy.wait()
            product = lax.dot_general(wbuf[at, 0:deep], x_ref[:, 0:deep], (((1,), (1,)), ((), ())),
                                      preferred_element_type=jnp.float32)
            if not final:
                for copy in weight_copies(p + 1, i):
                    copy.start()

                @pl.when(i == (tiles * 4) // 5)
                def _():
                    relay(p + 1)

            if p == 0:
                acc[at, :] = product
            elif not final:
                acc[at, :] = acc[at, :] + product
            else:
                logits = acc[at, :] + product
                row = lax.broadcasted_iota(jnp.int32, (tile, positions), 0) + i * tile
                hit = jnp.where(row == targets, logits, 0.0)
                sums[...] += jnp.sum(jnp.exp(logits).reshape(tile // 8, 8, positions), axis=0)
                picks[...] += jnp.sum(hit.reshape(tile // 8, 8, positions), axis=0)
            return carry

        lax.fori_loop(0, tiles, one_tile, 0)

    place = lax.broadcasted_iota(jnp.int32, (1, positions), 1)
    own_cols = columns // groups
    base = d * columns + v * own_cols
    own_ref = jnp.zeros((1, positions), jnp.float32)
    for j in range(own_cols):
        own_ref = jnp.where(place == base + j, jnp.broadcast_to(ref_v[0:1, j:j + 1], (1, positions)), own_ref)
    red[me] = jnp.concatenate(
        [jnp.sum(sums[...], axis=0, keepdims=True), jnp.sum(picks[...], axis=0, keepdims=True) - own_ref], axis=0)

    def share(k):
        peer = lax.rem(me + k, devices)
        return send(red.at[me], red.at[me], r_send.at[k], r_recv.at[me], (lax.div(peer, groups), lax.rem(peer, groups)))

    def send_share(k, carry):
        share(k).start()
        return carry

    lax.fori_loop(1, devices, send_share, 0)
    weights_mask = spread(1).astype(jnp.float32)

    for k in range(1, seqs):
        to_plane(k).wait_send()
        meta_to(k).wait_send()
    for zc in range(depth):
        for dc in range(seqs):
            to_partner(zc, dc).wait_send()

            @pl.when(has_above & (z >= zc))
            def _():
                to_above(zc, dc).wait_send()

            @pl.when(has_below & (z <= zc))
            def _():
                to_below(zc, dc).wait_send()

    def take_share(k, carry):
        peer = lax.rem(me + k, devices)
        send(red.at[peer], red.at[peer], r_send.at[k], r_recv.at[peer], partner).wait_recv()
        return carry

    lax.fori_loop(1, devices, take_share, 0)
    total = jnp.sum(red[...], axis=0)
    log_partition = jnp.log(total[0:1])
    differences = weights_mask * (total[1:2] - log_partition)
    own_logps = (total[1:2] + own_ref) - log_partition
    row8 = lax.broadcasted_iota(jnp.int32, (own_cols, positions), 0)
    lane8 = lax.broadcasted_iota(jnp.int32, (own_cols, positions), 1)
    out[0:own_cols, :] = jnp.broadcast_to(
        jnp.sum(jnp.where(lane8 == base + row8, own_logps, 0.0), axis=1, keepdims=True), (own_cols, LANES))
    within = lax.rem(place, columns)
    kl_total = jnp.sum(jnp.where(within >= length, differences, 0.0), axis=1, keepdims=True)
    mean_loss = jnp.zeros((1, 1), jnp.float32)
    own_loss = jnp.zeros((1, 1), jnp.float32)
    for s in range(seqs):
        mine = (place >= s * columns) & (place < s * columns + length)
        logratio = jnp.sum(jnp.where(mine, differences, 0.0), axis=1, keepdims=True)
        shift = kto_beta * (logratio - kl_total / seqs)
        wanted = desirable_weight * (1.0 - 1.0 / (1.0 + jnp.exp(-shift)))
        unwanted = undesirable_weight * (1.0 - 1.0 / (1.0 + jnp.exp(shift)))
        one = jnp.where(meta[s, 3:4, 0:1] == 1, wanted, unwanted)
        mean_loss = mean_loss + one
        own_loss = jnp.where(d == s, one, own_loss)
    out[own_cols:own_cols + 1, :] = jnp.broadcast_to(own_loss, (1, LANES))
    out[own_cols + 1:own_cols + 2, :] = jnp.broadcast_to(mean_loss / seqs, (1, LANES))

    def end_share(k, carry):
        share(k).wait_send()
        return carry

    lax.fori_loop(1, devices, end_share, 0)


def fused(dims, hidden, kl_hidden, head_weight, labels, token_mask, kl_pair, desirable, ref_logps):
    seqs, groups = dims
    depth = groups // 2
    length, width = hidden.shape[1], hidden.shape[2]
    columns = 2 * length
    positions = seqs * columns
    chunk = 2 * width
    vocab_rows = head_weight.shape[0]
    tiles = vocab_rows // TILE_ROWS
    own_cols = columns // groups
    devices = seqs * groups
    dma = pltpu.SemaphoreType.DMA
    result = pl.pallas_call(
        functools.partial(fused_kernel, dims),
        name="kto_head",
        out_shape=jax.ShapeDtypeStruct((own_cols + 8, LANES), jnp.float32),
        in_specs=[pl.BlockSpec(memory_space=pltpu.HBM)] * 8,
        out_specs=pl.BlockSpec(memory_space=pltpu.VMEM),
        scratch_shapes=[
            pltpu.VMEM((2, depth, positions, width), jnp.bfloat16),
            pltpu.VMEM((vocab_rows, chunk + LANES), jnp.bfloat16),
            pltpu.VMEM((vocab_rows, positions), jnp.float32),
            pltpu.VMEM((positions, chunk), jnp.bfloat16),
            pltpu.VMEM((positions, chunk + LANES), jnp.bfloat16),
            pltpu.VMEM((1, length), jnp.int32),
            pltpu.VMEM((1, length), jnp.int32),
            pltpu.VMEM((1, 1), jnp.int32),
            pltpu.VMEM((1, 1), jnp.int32),
            pltpu.VMEM((1, own_cols), jnp.float32),
            pltpu.VMEM((seqs, 8, LANES), jnp.int32),
            pltpu.VMEM((8, positions), jnp.float32),
            pltpu.VMEM((8, positions), jnp.float32),
            pltpu.VMEM((devices, 2, positions), jnp.float32),
            dma((2,)),
            dma((5,)),
            dma((tiles, 2)),
            dma((depth, seqs)),
            dma((depth, seqs)),
            dma((seqs,)),
            dma((depth, seqs)),
            dma((depth, seqs)),
            dma((depth, seqs)),
            dma((seqs,)),
            dma((seqs,)),
            dma((devices,)),
            dma((devices,)),
        ],
        compiler_params=pltpu.CompilerParams(
            collective_id=0, has_side_effects=True, vmem_limit_bytes=60 * 1024 * 1024),
    )(hidden, kl_hidden, head_weight, labels, token_mask, kl_pair.reshape(1, 1), desirable.reshape(1, 1), ref_logps)
    return result[0:own_cols, 0].reshape(1, own_cols), result[own_cols, 0:1], result[own_cols + 1, 0]


def on_device(dims, *arrays):
    hidden, head_weight = arrays[0], arrays[2]
    seqs, groups = dims
    fits = (
        hidden.shape[0] == 1
        and seqs % 2 == 0
        and groups % 4 == 0
        and 4 * hidden.shape[1] == LANES
        and (2 * hidden.shape[2]) % (2 * LANES) == LANES
        and head_weight.shape[0] % TILE_ROWS == 0
        and (2 * hidden.shape[1]) % groups == 0
    )
    return fused(dims, *arrays) if fits else gathered_by_xla(*arrays)


def solution(mesh):
    in_specs = (
        P("dp", None, "vocab"),
        P("dp", None, "vocab"),
        P(("dp", "vocab"), None),
        P("dp", None),
        P("dp", None),
        P("dp"),
        P("dp"),
        P("dp", "vocab"),
    )
    out_specs = (P("dp", "vocab"), P("dp"), P())
    return jax.shard_map(
        functools.partial(on_device, tuple(mesh.shape[a] for a in ("dp", "vocab"))), mesh=mesh, in_specs=in_specs, out_specs=out_specs, check_vma=False
    )
```
